32 devices in a mesh: gx: 4 (over z), gy: 2 (over x), gz: 4 (over y, core).
Axes of the slice: x: 2, y: 2, z: 4, core: 2. Of those that a mesh axis runs over, the one named last changes fastest.
Arguments:
- volume: bfloat16 [32, 8, 32, 512], P(None, 'gx', 'gy', 'gz'), may hold values from -6 to 6
- w_first: bfloat16 [3, 3, 3, 32, 32], replicated, may hold values from -0.21875 to 0.21875
- w_second: bfloat16 [3, 3, 3, 32, 32], replicated, may hold values from -0.21875 to 0.21875
- v_first: bfloat16 [3, 3, 3, 32, 32], replicated, may hold values from -0.21875 to 0.21875
- v_second: bfloat16 [3, 3, 3, 32, 32], replicated, may hold values from -0.21875 to 0.21875
Outputs:
- jv: bfloat16 [32, 8, 32, 512], P(None, 'gx', 'gy', 'gz')
- gv_first: float32 [3, 3, 3, 32, 32], replicated
- gv_second: float32 [3, 3, 3, 32, 32], replicated
The draws below stay inside these ranges and needn't reach their ends.
All inputs are finite; a program needn't handle non-finite values.
Results may differ from the reference program's by a relative error of at most 0.005.
Values may be sent and summed in bfloat16 or wider, within the bound.
A program may use at most 64 MiB of HBM per device.

```python
import jax
import jax.numpy as jnp
from jax import lax

CHANNELS = 32
NX = 8
NY = 32
NZ = 512
CELLS = 131072
FILT = 864


def shard_levels(key, extent, split, least, high):
    factor_of, own = 1.0, jax.random.fold_in(key, 6)
    for dim, parts in split:
        heights = jnp.exp(jax.random.uniform(jax.random.fold_in(own, dim), (parts,), jnp.float32, least / len(split), high / len(split)))
        factor_of = factor_of * jnp.repeat(heights, extent[dim] // parts).reshape([-1 if axis == dim else 1 for axis in range(len(extent))])
    return factor_of


def bell_draw(key, dims, deviation, bound, shards=(), held_as=jnp.bfloat16):
    gain = shard_levels(key, dims, shards, -0.22, 0.18) if shards else 1.0
    drawn = jax.random.normal(key, dims, jnp.float32) * deviation * gain
    return jnp.minimum(jnp.maximum(drawn, -bound), bound).astype(held_as)


def setup_inputs(seed: int = 0) -> dict:
    key_of = jax.random.split(jax.random.key(seed), 6)
    return {
        "volume": bell_draw(key_of[0], (CHANNELS, NX, NY, NZ), 1.0, 6.0, ((1, 4), (2, 2), (3, 4))),
        "w_first": bell_draw(key_of[1], (3, 3, 3, CHANNELS, CHANNELS), FILT ** -0.5, 0.21875),
        "w_second": bell_draw(key_of[2], (3, 3, 3, CHANNELS, CHANNELS), FILT ** -0.5, 0.21875),
        "v_first": bell_draw(key_of[3], (3, 3, 3, CHANNELS, CHANNELS), FILT ** -0.5, 0.21875),
        "v_second": bell_draw(key_of[4], (3, 3, 3, CHANNELS, CHANNELS), FILT ** -0.5, 0.21875),
    }


def gelu_pair(pre):
    inner = 0.7978845608 * (pre + 0.044715 * pre * pre * pre)
    hyper = jnp.tanh(inner)
    hidden = 0.5 * pre * (1.0 + hyper)
    slope = 0.5 * (1.0 + hyper) + 0.5 * pre * (1.0 - hyper * hyper) * 0.7978845608 * (1.0 + 0.134145 * pre * pre)
    return hidden, slope


def convolve(field, weight):
    result = lax.conv_general_dilated(field.astype(jnp.float32)[None], weight.astype(jnp.float32), (1, 1, 1), "SAME", dimension_numbers=("NCDHW", "DHWIO", "NCDHW"), precision=lax.Precision.HIGHEST)
    return result[0]


def correlate(field, target):
    padded = jnp.pad(field.astype(jnp.float32), ((0, 0), (1, 1), (1, 1), (1, 1)))
    target32 = target.astype(jnp.float32)
    sizes = field.shape
    planes = []
    for shift_x in range(3):
        rows_y = []
        for shift_y in range(3):
            rows_z = []
            for shift_z in range(3):
                window = padded[:, shift_x:shift_x + sizes[1], shift_y:shift_y + sizes[2], shift_z:shift_z + sizes[3]]
                rows_z.append(jnp.einsum("cxyz,oxyz->co", window, target32, precision=lax.Precision.HIGHEST))
            rows_y.append(jnp.stack(rows_z))
        planes.append(jnp.stack(rows_y))
    return jnp.stack(planes)


def reference(volume, w_first, w_second, v_first, v_second):
    pre = convolve(volume, w_first)
    hidden_f, slope = gelu_pair(pre)
    hidden = hidden_f.astype(jnp.bfloat16)
    tangent = (slope * convolve(volume, v_first)).astype(jnp.bfloat16)
    jv = (convolve(tangent, w_second) + convolve(hidden, v_second)).astype(jnp.bfloat16)
    flipped = jnp.transpose(jnp.flip(w_second, (0, 1, 2)), (0, 1, 2, 4, 3))
    back = (slope * convolve(jv, flipped)).astype(jnp.bfloat16)
    count_all = jnp.float32(CELLS)
    factor = jnp.float32(FILT) ** 0.5
    gv_second = factor * (correlate(hidden, jv) / count_all + 0.1 * v_second.astype(jnp.float32))
    gv_first = factor * (correlate(volume, back) / count_all + 0.1 * v_first.astype(jnp.float32))
    return jv, gv_first, gv_second
```

```python
import functools
import itertools
import math

import jax
import jax.numpy as jnp
from jax import lax
from jax.experimental import pallas as pl
from jax.experimental.pallas import tpu as pltpu
from jax.sharding import PartitionSpec as P

MESH = pl.DeviceIdType.MESH
AXES = ("gx", "gy", "gz")
STEPS = [d for d in itertools.product((-1, 0, 1), repeat=3) if d != (0, 0, 0)]
STEPS.sort(key=lambda d: (d[2] != 0, d[0] == 0, abs(d[0]) + abs(d[1])))
NT = (((1,), (1,)), ((), ()))


def gelu_pair(pre):
    inner = 0.7978845608 * (pre + 0.044715 * pre * pre * pre)
    hyper = jnp.tanh(inner)
    hidden = 0.5 * pre * (1.0 + hyper)
    slope = 0.5 * (1.0 + hyper) + 0.5 * pre * (1.0 - hyper * hyper) * 0.7978845608 * (
        1.0 + 0.134145 * pre * pre
    )
    return hidden, slope


def code(step):
    return (step[0] + 1) * 9 + (step[1] + 1) * 3 + step[2] + 1


def kernel(
    sizes,
    volume,
    w1,
    w2,
    w3,
    jv_out,
    gv1,
    gv2,
    *scratch,
):
    (rv, rp, rj, zv, zp, zj, ev, ep, ej, sv, sp, slope_ref, back_ref, acc, pack, land, part, full,
     hsend, hrecv, asend, arecv, bsend, brecv) = scratch
    depth, height, chan, width = volume.shape
    me = tuple(lax.axis_index(a) for a in AXES)
    total = sizes[0] * sizes[1] * sizes[2]
    line = (me[0] * sizes[1] + me[1]) * sizes[2] + me[2]

    def place(index):
        return (
            index // (sizes[1] * sizes[2]),
            index // sizes[2] % sizes[1],
            index % sizes[2],
        )

    barrier = pltpu.get_barrier_semaphore()

    @pl.loop(1, total)
    def _(i):
        pl.semaphore_signal(
            barrier, inc=1, device_id=place(lax.rem(line + i, total)), device_id_type=MESH
        )

    def there(step):
        ok = None
        for pos, size, delta in zip(me, sizes, step):
            if delta == -1:
                term = pos > 0
            elif delta == 1:
                term = pos < size - 1
            else:
                continue
            ok = term if ok is None else jnp.logical_and(ok, term)
        return ok

    def source(delta, extent):
        return {-1: pl.ds(1, 1), 1: pl.ds(extent, 1), 0: pl.ds(1, extent)}[delta]

    def target(delta, extent):
        return {-1: pl.ds(extent + 1, 1), 1: pl.ds(0, 1), 0: pl.ds(1, extent)}[delta]

    def landing(step, rows, zbuf):
        if step[2] == 0:
            return rows.at[target(step[0], depth), target(step[1], height)]
        return zbuf.at[0 if step[2] == 1 else 1, 1 - step[0], 1 - step[1]]

    def message(step, rows, zbuf, edge, slot):
        if step[2] == 0:
            src = rows.at[source(step[0], depth), source(step[1], height)]
        else:
            src = edge
        return pltpu.make_async_remote_copy(
            src_ref=src,
            dst_ref=landing(step, rows, zbuf),
            send_sem=hsend.at[slot, code(step)],
            recv_sem=hrecv.at[slot, code(step)],
            device_id=tuple(p + d for p, d in zip(me, step)),
            device_id_type=MESH,
        )

    def send(rows, zbuf, edge, slot, cross):
        for step in STEPS:
            if (step[2] != 0) == cross:

                @pl.when(there(step))
                def _():
                    message(step, rows, zbuf, edge, slot).start()

    def clear(rows, zbuf):
        for step in STEPS:
            back = tuple(-d for d in step)

            @pl.when(jnp.logical_not(there(back)))
            def _():
                ref = landing(step, rows, zbuf)
                ref[...] = jnp.zeros(ref.shape, ref.dtype)

    def receive(rows, zbuf, edge, slot):
        for step in STEPS:
            back = tuple(-d for d in step)

            @pl.when(there(back))
            def _():
                message(step, rows, zbuf, edge, slot).wait_recv()

    def sent(rows, zbuf, edge, slot):
        for step in STEPS:

            @pl.when(there(step))
            def _():
                message(step, rows, zbuf, edge, slot).wait_send()

    def edges(rows, edge):
        count = rows.shape[2]
        lane = lax.broadcasted_iota(jnp.int32, (count, width), 1)
        cells = depth * height
        built = jnp.zeros((count, width), jnp.float32)
        for x in range(depth):

            def step(y, built, x=x):
                row = rows[x + 1, y + 1].astype(jnp.float32)
                at = x * height + y
                built = jnp.where(lane == at, pltpu.roll(row, at, 1), built)
                return jnp.where(lane == cells + at, pltpu.roll(row, cells + at + 1, 1), built)

            built = lax.fori_loop(0, height, step, built, unroll=4)
        edge[...] = built.astype(edge.dtype)

    def spread(rows, zbuf, out):
        count = rows.shape[2]
        groups = count // chan
        lane = lax.broadcasted_iota(jnp.int32, (count, width), 1)
        cells = depth * height

        def one(xp, yp, dy, y):
            dx = 0 if xp == 0 else (2 if xp == depth + 1 else 1)
            at = (xp - 1) % depth * height + y
            row = rows[xp, yp]
            wide = row.astype(jnp.float32)
            left = zbuf[0, dx, dy].astype(jnp.float32)
            right = zbuf[1, dx, dy].astype(jnp.float32)
            low = jnp.where(
                lane == 0,
                pltpu.roll(left, width - cells - at, 1),
                pltpu.roll(wide, 1, 1),
            ).astype(row.dtype)
            high = jnp.where(
                lane == width - 1,
                pltpu.roll(right, width - 1 - at, 1),
                pltpu.roll(wide, width - 1, 1),
            ).astype(row.dtype)
            for g in range(groups):
                part_of = slice(g * chan, (g + 1) * chan)
                base = g * 3 * chan
                out[xp, yp, base : base + chan] = low[part_of]
                out[xp, yp, base + chan : base + 2 * chan] = row[part_of]
                out[xp, yp, base + 2 * chan : base + 3 * chan] = high[part_of]

        for xp in range(depth + 2):
            one(xp, 0, 0, height - 1)
            one(xp, height + 1, 2, 0)

            @pl.loop(0, height, unroll=2)
            def _(y, xp=xp):
                one(xp, y + 1, 1, y)

    def window(ref, x, y, span):
        return ref[pl.ds(x, span), pl.ds(y, 3)].reshape(span * 3 * ref.shape[2], width)

    def convolve(weights, ref, finish):
        for x in range(depth):

            @pl.loop(0, height // 2)
            def _(j, x=x):
                y = 2 * j
                rhs = jnp.concatenate([window(ref, x, y, 3), window(ref, x, y + 1, 3)], axis=1)
                out = jnp.dot(weights[...], rhs, preferred_element_type=jnp.float32)
                finish(x, y, out[:, :width])
                finish(x, y + 1, out[:, width:])

    def correlate(ref, rows, offset):
        acc[...] = jnp.zeros_like(acc)
        for x in range(depth):

            @pl.loop(0, height // 4)
            def _(j, x=x):
                y = 4 * j
                rhs = jnp.concatenate(
                    [rows[x + offset, y + i + offset] for i in range(4)], axis=1
                )
                for kx in range(3):
                    lhs = jnp.concatenate(
                        [
                            ref[x + kx, pl.ds(y + i, 3), : 3 * chan].reshape(9 * chan, width)
                            for i in range(4)
                        ],
                        axis=1,
                    )
                    acc[kx] += lax.dot_general(lhs, rhs, NT, preferred_element_type=jnp.float32)

    tiles = pack.shape[1]

    def owner(t):
        return t * total // tiles

    span = 8 * tiles
    lanes = width // chan

    def scatter(slot):
        for j in range(lanes):
            flat = acc[...].reshape(27 * chan, chan)
            pack[slot, :, :, j * chan : (j + 1) * chan] = flat[
                j * span : (j + 1) * span
            ].reshape(tiles, 8, chan)
        for t in range(tiles):
            at = owner(t)

            @pl.when(line != at)
            def _():
                pltpu.make_async_remote_copy(
                    src_ref=pack.at[slot, t],
                    dst_ref=land.at[slot, lax.rem(line - at + total, total) - 1],
                    send_sem=asend.at[slot],
                    recv_sem=arecv.at[slot],
                    device_id=place(at),
                    device_id_type=MESH,
                ).start()

    def gather(slot):
        for t in range(tiles):

            @pl.when(line == owner(t))
            def _():
                pltpu.make_async_copy(
                    land.at[slot], land.at[slot], arecv.at[slot]
                ).wait()
                summed = pack[slot, t] + jnp.sum(land[slot], axis=0)
                part[slot] = summed
                full[slot, t] = summed

                @pl.loop(1, total)
                def _(i):
                    pltpu.make_async_remote_copy(
                        src_ref=part.at[slot],
                        dst_ref=full.at[slot, t],
                        send_sem=bsend.at[slot],
                        recv_sem=brecv.at[slot],
                        device_id=place(lax.rem(line + i, total)),
                        device_id_type=MESH,
                    ).start()

    def owning():
        held = line == owner(0)
        for t in range(1, tiles):
            held = jnp.logical_or(held, line == owner(t))
        return held

    def drain(slot, out):
        held = owning()
        for flag, count in ((held, tiles - 1), (jnp.logical_not(held), tiles)):

            @pl.when(flag)
            def _():
                some = full.at[slot, pl.ds(0, count)]
                pltpu.make_async_copy(some, some, brecv.at[slot]).wait()
                mine = pack.at[slot, pl.ds(0, count)]
                pltpu.make_async_copy(mine, mine, asend.at[slot]).wait()

        @pl.when(held)
        def _():
            pltpu.make_async_copy(land.at[slot], land.at[slot], bsend.at[slot]).wait()

        whole = full[slot].reshape(span, width)
        for j in range(lanes):
            out[j * span : (j + 1) * span] = whole[:, j * chan : (j + 1) * chan]

    inner = (slice(1, depth + 1), slice(1, height + 1))
    rv[inner] = volume[...]
    edges(rv, ev)
    for rows, zbuf in ((rv, zv), (rp, zp), (rj, zj)):
        clear(rows, zbuf)
    pl.semaphore_wait(barrier, total - 1)

    send(rv, zv, ev, 0, False)
    send(rv, zv, ev, 0, True)
    receive(rv, zv, ev, 0)
    spread(rv, zv, sv)

    def first(x, y, out):
        hidden, slope = gelu_pair(out[:chan])
        slope_ref[x, y] = slope
        rp[x + 1, y + 1, :chan] = hidden.astype(jnp.bfloat16)
        rp[x + 1, y + 1, chan:] = (slope * out[chan:]).astype(jnp.bfloat16)

    convolve(w1, sv, first)
    send(rp, zp, ep, 1, False)
    edges(rp, ep)
    send(rp, zp, ep, 1, True)
    receive(rp, zp, ep, 1)
    spread(rp, zp, sp)

    def second(x, y, out):
        rj[x + 1, y + 1] = out.astype(jnp.bfloat16)

    convolve(w2, sp, second)
    send(rj, zj, ej, 2, False)
    edges(rj, ej)
    send(rj, zj, ej, 2, True)
    jv_out[...] = rj[inner]
    correlate(sp, rj, 1)
    scatter(0)
    receive(rj, zj, ej, 2)
    sj = sp.at[:, :, : 3 * chan]
    spread(rj, zj, sj)

    def third(x, y, out):
        back_ref[x, y] = (slope_ref[x, y] * out).astype(jnp.bfloat16)

    convolve(w3, sj, third)
    gather(0)
    correlate(sv, back_ref, 0)
    scatter(1)
    gather(1)
    drain(0, gv2)
    drain(1, gv1)
    sent(rv, zv, ev, 0)
    sent(rp, zp, ep, 1)
    sent(rj, zj, ej, 2)


def body(volume, w_first, w_second, v_first, v_second):
    chan, depth, height, width = volume.shape
    sizes = tuple(lax.axis_size(a) for a in AXES)
    total = sizes[0] * sizes[1] * sizes[2]
    filt = 27 * chan
    tiles = filt * chan // (8 * width)
    w1 = jnp.concatenate([w_first, v_first], axis=-1).reshape(filt, 2 * chan).T
    w2 = jnp.stack([v_second, w_second], axis=2).reshape(2 * filt, chan).T
    w3 = jnp.transpose(jnp.flip(w_second, (0, 1, 2)), (3, 0, 1, 2, 4)).reshape(chan, filt)
    cells = jnp.transpose(volume, (1, 2, 0, 3))
    bf, f32 = jnp.bfloat16, jnp.float32
    pads = (depth + 2, height + 2)
    vmem = pl.BlockSpec(memory_space=pltpu.VMEM)
    jv, corr1, corr2 = pl.pallas_call(
        functools.partial(kernel, sizes),
        out_shape=(
            jax.ShapeDtypeStruct((depth, height, chan, width), bf),
            jax.ShapeDtypeStruct((filt, chan), f32),
            jax.ShapeDtypeStruct((filt, chan), f32),
        ),
        in_specs=[vmem] * 4,
        out_specs=(vmem,) * 3,
        scratch_shapes=[
            pltpu.VMEM(pads + (chan, width), bf),
            pltpu.VMEM(pads + (2 * chan, width), bf),
            pltpu.VMEM(pads + (chan, width), bf),
            pltpu.VMEM((2, 3, 3, chan, width), bf),
            pltpu.VMEM((2, 3, 3, 2 * chan, width), bf),
            pltpu.VMEM((2, 3, 3, chan, width), bf),
            pltpu.VMEM((chan, width), bf),
            pltpu.VMEM((2 * chan, width), bf),
            pltpu.VMEM((chan, width), bf),
            pltpu.VMEM(pads + (3 * chan, width), bf),
            pltpu.VMEM(pads + (6 * chan, width), bf),
            pltpu.VMEM((depth, height, chan, width), f32),
            pltpu.VMEM((depth, height, chan, width), bf),
            pltpu.VMEM((3, 9 * chan, chan), f32),
            pltpu.VMEM((2, tiles, 8, width), f32),
            pltpu.VMEM((2, total - 1, 8, width), f32),
            pltpu.VMEM((2, 8, width), f32),
            pltpu.VMEM((2, tiles, 8, width), f32),
            pltpu.SemaphoreType.DMA((3, 27)),
            pltpu.SemaphoreType.DMA((3, 27)),
            pltpu.SemaphoreType.DMA((2,)),
            pltpu.SemaphoreType.DMA((2,)),
            pltpu.SemaphoreType.DMA((2,)),
            pltpu.SemaphoreType.DMA((2,)),
        ],
        compiler_params=pltpu.CompilerParams(
            collective_id=0, has_side_effects=True, vmem_limit_bytes=48 * 1024 * 1024
        ),
    )(cells, w1, w2, w3)
    count = float(depth * height * width * total)
    factor = math.sqrt(27.0 * chan)
    gv_first = factor * (corr1.reshape(v_first.shape) / count + 0.1 * v_first.astype(f32))
    gv_second = factor * (corr2.reshape(v_second.shape) / count + 0.1 * v_second.astype(f32))
    return jnp.transpose(jv, (2, 0, 1, 3)), gv_first, gv_second


def solution(mesh):
    in_specs = (P(None, "gx", "gy", "gz"), P(), P(), P(), P())
    out_specs = (P(None, "gx", "gy", "gz"), P(), P())
    return jax.shard_map(body, mesh=mesh, in_specs=in_specs, out_specs=out_specs, check_vma=False)
```

```python
import functools
import itertools
import math

import jax
import jax.numpy as jnp
from jax import lax
from jax.experimental import pallas as pl
from jax.experimental.pallas import tpu as pltpu
from jax.sharding import PartitionSpec as P

MESH = pl.DeviceIdType.MESH
AXES = ("gx", "gy", "gz")
STEPS = [d for d in itertools.product((-1, 0, 1), repeat=3) if d != (0, 0, 0)]
STEPS.sort(key=lambda d: (d[2] != 0, d[0] == 0, abs(d[0]) + abs(d[1])))
NT = (((1,), (1,)), ((), ()))


def gelu_pair(pre):
    inner = 0.7978845608 * (pre + 0.044715 * pre * pre * pre)
    hyper = jnp.tanh(inner)
    hidden = 0.5 * pre * (1.0 + hyper)
    slope = 0.5 * (1.0 + hyper) + 0.5 * pre * (1.0 - hyper * hyper) * 0.7978845608 * (
        1.0 + 0.134145 * pre * pre
    )
    return hidden, slope


def code(step):
    return (step[0] + 1) * 9 + (step[1] + 1) * 3 + step[2] + 1


def kernel(
    sizes,
    volume,
    w1,
    w2,
    w3,
    jv_out,
    gv1,
    gv2,
    *scratch,
):
    (rv, rp, rj, zv, zp, zj, ev, ep, ej, sv, sp, sj, slope_ref, back_ref,
     t1, t2, t3, shift, keep, acc, pack, land, part, full,
     hsend, hrecv, asend, arecv, bsend, brecv) = scratch
    depth, height, chan, width = volume.shape
    me = tuple(lax.axis_index(a) for a in AXES)
    total = sizes[0] * sizes[1] * sizes[2]
    line = (me[0] * sizes[1] + me[1]) * sizes[2] + me[2]

    def place(index):
        return (
            index // (sizes[1] * sizes[2]),
            index // sizes[2] % sizes[1],
            index % sizes[2],
        )

    barrier = pltpu.get_barrier_semaphore()

    @pl.loop(1, total)
    def _(i):
        pl.semaphore_signal(
            barrier, inc=1, device_id=place(lax.rem(line + i, total)), device_id_type=MESH
        )

    def there(step):
        ok = None
        for pos, size, delta in zip(me, sizes, step):
            if delta == -1:
                term = pos > 0
            elif delta == 1:
                term = pos < size - 1
            else:
                continue
            ok = term if ok is None else jnp.logical_and(ok, term)
        return ok

    def source(delta, extent):
        return {-1: pl.ds(1, 1), 1: pl.ds(extent, 1), 0: pl.ds(1, extent)}[delta]

    def target(delta, extent):
        return {-1: pl.ds(extent + 1, 1), 1: pl.ds(0, 1), 0: pl.ds(1, extent)}[delta]

    def landing(step, rows, zbuf):
        if step[2] == 0:
            return rows.at[target(step[0], depth), target(step[1], height)]
        return zbuf.at[0 if step[2] == 1 else 1, 1 - step[0], 1 - step[1]]

    def message(step, rows, zbuf, edge, slot):
        if step[2] == 0:
            src = rows.at[source(step[0], depth), source(step[1], height)]
        else:
            src = edge
        return pltpu.make_async_remote_copy(
            src_ref=src,
            dst_ref=landing(step, rows, zbuf),
            send_sem=hsend.at[slot, code(step)],
            recv_sem=hrecv.at[slot, code(step)],
            device_id=tuple(p + d for p, d in zip(me, step)),
            device_id_type=MESH,
        )

    def send(rows, zbuf, edge, slot, cross):
        for step in STEPS:
            if (step[2] != 0) == cross:

                @pl.when(there(step))
                def _():
                    message(step, rows, zbuf, edge, slot).start()

    def clear(rows, zbuf):
        for step in STEPS:
            back = tuple(-d for d in step)

            @pl.when(jnp.logical_not(there(back)))
            def _():
                ref = landing(step, rows, zbuf)
                ref[...] = jnp.zeros(ref.shape, ref.dtype)

    def receive(rows, zbuf, edge, slot, kind):
        for step in STEPS:
            if (step[0] != 0) != (kind == 1):
                continue
            back = tuple(-d for d in step)

            @pl.when(there(back))
            def _():
                message(step, rows, zbuf, edge, slot).wait_recv()

    def stage(rows, zbuf, edge, slot, out, table, group, finish):
        for kind in range(2):
            receive(rows, zbuf, edge, slot, kind)
            spread(rows, zbuf, out, (near, far)[kind])
            convolve(table, out, group, kind, finish)

    def sent(rows, zbuf, edge, slot):
        for step in STEPS:

            @pl.when(there(step))
            def _():
                message(step, rows, zbuf, edge, slot).wait_send()

    def edges(rows, edge):
        count = rows.shape[2]
        lane = lax.broadcasted_iota(jnp.int32, (count, width), 1)
        cells = depth * height
        built = jnp.zeros((count, width), jnp.float32)
        for x in range(depth):

            def step(y, built, x=x):
                row = rows[x + 1, y + 1].astype(jnp.float32)
                at = x * height + y
                built = jnp.where(lane == at, pltpu.roll(row, at, 1), built)
                return jnp.where(lane == cells + at, pltpu.roll(row, cells + at + 1, 1), built)

            built = lax.fori_loop(0, height, step, built, unroll=4)
        edge[...] = built.astype(edge.dtype)

    def shifter():
        src = lax.broadcasted_iota(jnp.int32, (2 * width, 2 * width), 0)
        dst = lax.broadcasted_iota(jnp.int32, (2 * width, 2 * width), 1)
        cells = depth * height
        low = jnp.logical_or(
            jnp.logical_and(src == dst - 1, src < width - 1),
            jnp.logical_and(
                dst == 0, jnp.logical_and(src >= width + cells, src < width + 2 * cells)
            ),
        )
        high = jnp.logical_or(
            jnp.logical_and(src == dst - width + 1, src < width),
            jnp.logical_and(
                dst == 2 * width - 1, jnp.logical_and(src >= width, src < width + cells)
            ),
        )
        pick = jnp.logical_or(
            jnp.logical_and(dst < width, low), jnp.logical_and(dst >= width, high)
        )
        shift[...] = jnp.where(pick, 1.0, 0.0).astype(shift.dtype)

    near = tuple(range(1, depth + 1))
    far = (0, depth + 1)

    def spread(rows, zbuf, out, planes):
        count = rows.shape[2]
        groups = count // chan
        lane = lax.broadcasted_iota(jnp.int32, (count, width), 1)
        cells = depth * height

        def block(xp, yp, dy, y, many):
            dx = 0 if xp == 0 else (2 if xp == depth + 1 else 1)
            left = zbuf[0, dx, dy].astype(jnp.float32)
            right = zbuf[1, dx, dy].astype(jnp.float32)
            halo = []
            for i in range(many):
                at = (xp - 1) % depth * height + y + i
                both = jnp.where(lane == at, right, jnp.where(lane == cells + at, left, 0.0))
                halo.append(both.astype(rows.dtype))
            wide = rows[xp, pl.ds(yp, many)].reshape(many * count, width)
            lhs = jnp.concatenate([wide, jnp.concatenate(halo, axis=0)], axis=1)
            moved = jnp.dot(lhs, shift[...], preferred_element_type=jnp.float32)
            moved = moved.astype(rows.dtype)
            for i in range(many):
                for g in range(groups):
                    at = slice(i * count + g * chan, i * count + (g + 1) * chan)
                    base = g * 3 * chan
                    out[xp, yp + i, base : base + chan] = moved[at, :width]
                    out[xp, yp + i, base + chan : base + 2 * chan] = wide[at]
                    out[xp, yp + i, base + 2 * chan : base + 3 * chan] = moved[at, width:]

        many = 4 // groups
        for xp in planes:
            block(xp, 0, 0, height - 1, 1)
            block(xp, height + 1, 2, 0, 1)

            @pl.loop(0, height // many)
            def _(j, xp=xp):
                block(xp, many * j + 1, 1, many * j, many)

    def band(weights, table, group):
        outs = weights.shape[0]
        third = weights.shape[1] // 3
        step = third // 3
        table[...] = jnp.zeros_like(table)
        for kx in range(3):
            piece = weights[:, kx * third : (kx + 1) * third]
            for ox in range(depth):
                xp = ox + kx
                kind, pos = (0, near.index(xp)) if xp in near else (1, far.index(xp))
                for oy in range(group):
                    row = (ox * group + oy) * outs
                    at = (pos * (group + 2) + oy) * step
                    table[kind, row : row + outs, at : at + third] = piece

    def convolve(table, ref, group, kind, finish):
        outs = table.shape[1] // (depth * group)
        planes = (near, far)[kind]

        @pl.loop(0, height // (2 * group))
        def _(j):
            halves = []
            for half in range(2):
                y = (2 * j + half) * group
                halves.append(
                    jnp.concatenate(
                        [
                            ref[xp, pl.ds(y, group + 2)].reshape(
                                (group + 2) * ref.shape[2], width
                            )
                            for xp in planes
                        ],
                        axis=0,
                    )
                )
            rhs = jnp.concatenate(halves, axis=1)
            out = jnp.dot(
                table[kind, :, : rhs.shape[0]], rhs, preferred_element_type=jnp.float32
            )
            if kind == 0:
                keep[j] = out
                return
            out = out + keep[j]
            for half in range(2):
                for ox in range(depth):
                    for oy in range(group):
                        row = (ox * group + oy) * outs
                        finish(
                            ox,
                            (2 * j + half) * group + oy,
                            out[row : row + outs, half * width : (half + 1) * width],
                        )

    def correlate(ref, rows, offset):
        acc[...] = jnp.zeros_like(acc)
        for x in range(depth):

            @pl.loop(0, height // 4)
            def _(j, x=x):
                y = 4 * j
                rhs = jnp.concatenate(
                    [rows[x + offset, y + i + offset] for i in range(4)], axis=1
                )
                for kx in range(3):
                    lhs = jnp.concatenate(
                        [
                            ref[x + kx, pl.ds(y + i, 3), : 3 * chan].reshape(9 * chan, width)
                            for i in range(4)
                        ],
                        axis=1,
                    )
                    acc[kx] += lax.dot_general(lhs, rhs, NT, preferred_element_type=jnp.float32)

    tiles = pack.shape[1]

    def owner(t):
        return t * total // tiles

    span = 8 * tiles
    lanes = width // chan

    def scatter(slot):
        for j in range(lanes):
            flat = acc[...].reshape(27 * chan, chan)
            pack[slot, :, :, j * chan : (j + 1) * chan] = flat[
                j * span : (j + 1) * span
            ].reshape(tiles, 8, chan)
        for t in range(tiles):
            at = owner(t)

            @pl.when(line != at)
            def _():
                pltpu.make_async_remote_copy(
                    src_ref=pack.at[slot, t],
                    dst_ref=land.at[slot, lax.rem(line - at + total, total) - 1],
                    send_sem=asend.at[slot],
                    recv_sem=arecv.at[slot],
                    device_id=place(at),
                    device_id_type=MESH,
                ).start()

    def gather(slot):
        for t in range(tiles):

            @pl.when(line == owner(t))
            def _():
                pltpu.make_async_copy(
                    land.at[slot], land.at[slot], arecv.at[slot]
                ).wait()
                summed = pack[slot, t] + jnp.sum(land[slot], axis=0)
                part[slot] = summed
                full[slot, t] = summed

                @pl.loop(1, total)
                def _(i):
                    pltpu.make_async_remote_copy(
                        src_ref=part.at[slot],
                        dst_ref=full.at[slot, t],
                        send_sem=bsend.at[slot],
                        recv_sem=brecv.at[slot],
                        device_id=place(lax.rem(line + i, total)),
                        device_id_type=MESH,
                    ).start()

    def owning():
        held = line == owner(0)
        for t in range(1, tiles):
            held = jnp.logical_or(held, line == owner(t))
        return held

    def drain(slot, out):
        held = owning()
        for flag, count in ((held, tiles - 1), (jnp.logical_not(held), tiles)):

            @pl.when(flag)
            def _():
                some = full.at[slot, pl.ds(0, count)]
                pltpu.make_async_copy(some, some, brecv.at[slot]).wait()
                mine = pack.at[slot, pl.ds(0, count)]
                pltpu.make_async_copy(mine, mine, asend.at[slot]).wait()

        @pl.when(held)
        def _():
            pltpu.make_async_copy(land.at[slot], land.at[slot], bsend.at[slot]).wait()

        whole = full[slot].reshape(span, width)
        for j in range(lanes):
            out[j * span : (j + 1) * span] = whole[:, j * chan : (j + 1) * chan]

    inner = (slice(1, depth + 1), slice(1, height + 1))
    rv[inner] = volume[...]
    edges(rv, ev)
    for rows, zbuf in ((rv, zv), (rp, zp), (rj, zj)):
        clear(rows, zbuf)
    pl.semaphore_wait(barrier, total - 1)
    send(rv, zv, ev, 0, False)
    send(rv, zv, ev, 0, True)
    shifter()
    band(w1, t1, 2)
    band(w2, t2, 4)
    band(w3, t3, 4)

    def first(x, y, out):
        hidden, slope = gelu_pair(out[:chan])
        slope_ref[x, y] = slope
        rp[x + 1, y + 1, :chan] = hidden.astype(jnp.bfloat16)
        rp[x + 1, y + 1, chan:] = (slope * out[chan:]).astype(jnp.bfloat16)

    stage(rv, zv, ev, 0, sv, t1, 2, first)
    send(rp, zp, ep, 1, False)
    edges(rp, ep)
    send(rp, zp, ep, 1, True)

    def second(x, y, out):
        rj[x + 1, y + 1] = out.astype(jnp.bfloat16)

    stage(rp, zp, ep, 1, sp, t2, 4, second)
    send(rj, zj, ej, 2, False)
    edges(rj, ej)
    send(rj, zj, ej, 2, True)
    jv_out[...] = rj[inner]
    correlate(sp, rj, 1)
    scatter(0)

    def third(x, y, out):
        back_ref[x, y] = (slope_ref[x, y] * out).astype(jnp.bfloat16)

    stage(rj, zj, ej, 2, sj, t3, 4, third)
    gather(0)
    correlate(sv, back_ref, 0)
    scatter(1)
    gather(1)
    drain(0, gv2)
    drain(1, gv1)
    sent(rv, zv, ev, 0)
    sent(rp, zp, ep, 1)
    sent(rj, zj, ej, 2)


def body(volume, w_first, w_second, v_first, v_second):
    chan, depth, height, width = volume.shape
    sizes = tuple(lax.axis_size(a) for a in AXES)
    total = sizes[0] * sizes[1] * sizes[2]
    filt = 27 * chan
    tiles = filt * chan // (8 * width)
    w1 = jnp.concatenate([w_first, v_first], axis=-1).reshape(filt, 2 * chan).T
    w2 = jnp.stack([v_second, w_second], axis=2).reshape(2 * filt, chan).T
    w3 = jnp.transpose(jnp.flip(w_second, (0, 1, 2)), (3, 0, 1, 2, 4)).reshape(chan, filt)
    cells = jnp.transpose(volume, (1, 2, 0, 3))
    bf, f32 = jnp.bfloat16, jnp.float32
    pads = (depth + 2, height + 2)
    vmem = pl.BlockSpec(memory_space=pltpu.VMEM)
    jv, corr1, corr2 = pl.pallas_call(
        functools.partial(kernel, sizes),
        out_shape=(
            jax.ShapeDtypeStruct((depth, height, chan, width), bf),
            jax.ShapeDtypeStruct((filt, chan), f32),
            jax.ShapeDtypeStruct((filt, chan), f32),
        ),
        in_specs=[vmem] * 4,
        out_specs=(vmem,) * 3,
        scratch_shapes=[
            pltpu.VMEM(pads + (chan, width), bf),
            pltpu.VMEM(pads + (2 * chan, width), bf),
            pltpu.VMEM(pads + (chan, width), bf),
            pltpu.VMEM((2, 3, 3, chan, width), bf),
            pltpu.VMEM((2, 3, 3, 2 * chan, width), bf),
            pltpu.VMEM((2, 3, 3, chan, width), bf),
            pltpu.VMEM((chan, width), bf),
            pltpu.VMEM((2 * chan, width), bf),
            pltpu.VMEM((chan, width), bf),
            pltpu.VMEM(pads + (3 * chan, width), bf),
            pltpu.VMEM(pads + (6 * chan, width), bf),
            pltpu.VMEM(pads + (3 * chan, width), bf),
            pltpu.VMEM((depth, height, chan, width), f32),
            pltpu.VMEM((depth, height, chan, width), bf),
            pltpu.VMEM((2, depth * 2 * 2 * chan, depth * 4 * 3 * chan), bf),
            pltpu.VMEM((2, depth * 4 * chan, depth * 6 * 6 * chan), bf),
            pltpu.VMEM((2, depth * 4 * chan, depth * 6 * 3 * chan), bf),
            pltpu.VMEM((2 * width, 2 * width), bf),
            pltpu.VMEM((height // 4, depth * 4 * chan, 2 * width), f32),
            pltpu.VMEM((3, 9 * chan, chan), f32),
            pltpu.VMEM((2, tiles, 8, width), f32),
            pltpu.VMEM((2, total - 1, 8, width), f32),
            pltpu.VMEM((2, 8, width), f32),
            pltpu.VMEM((2, tiles, 8, width), f32),
            pltpu.SemaphoreType.DMA((3, 27)),
            pltpu.SemaphoreType.DMA((3, 27)),
            pltpu.SemaphoreType.DMA((2,)),
            pltpu.SemaphoreType.DMA((2,)),
            pltpu.SemaphoreType.DMA((2,)),
            pltpu.SemaphoreType.DMA((2,)),
        ],
        compiler_params=pltpu.CompilerParams(
            collective_id=0, has_side_effects=True, vmem_limit_bytes=48 * 1024 * 1024
        ),
    )(cells, w1, w2, w3)
    count = float(depth * height * width * total)
    factor = math.sqrt(27.0 * chan)
    gv_first = factor * (corr1.reshape(v_first.shape) / count + 0.1 * v_first.astype(f32))
    gv_second = factor * (corr2.reshape(v_second.shape) / count + 0.1 * v_second.astype(f32))
    return jnp.transpose(jv, (2, 0, 1, 3)), gv_first, gv_second


def solution(mesh):
    in_specs = (P(None, "gx", "gy", "gz"), P(), P(), P(), P())
    out_specs = (P(None, "gx", "gy", "gz"), P(), P())
    return jax.shard_map(body, mesh=mesh, in_specs=in_specs, out_specs=out_specs, check_vma=False)
```

```python
import functools
import itertools
import math

import jax
import jax.numpy as jnp
from jax import lax
from jax.experimental import pallas as pl
from jax.experimental.pallas import tpu as pltpu
from jax.sharding import PartitionSpec as P

MESH = pl.DeviceIdType.MESH
AXES = ("gx", "gy", "gz")
STEPS = [d for d in itertools.product((-1, 0, 1), repeat=3) if d != (0, 0, 0)]
STEPS.sort(key=lambda d: (d[2] != 0, d[0] == 0, abs(d[0]) + abs(d[1])))
NT = (((1,), (1,)), ((), ()))


def gelu_pair(pre):
    inner = 0.7978845608 * (pre + 0.044715 * pre * pre * pre)
    hyper = jnp.tanh(inner)
    hidden = 0.5 * pre * (1.0 + hyper)
    slope = 0.5 * (1.0 + hyper) + 0.5 * pre * (1.0 - hyper * hyper) * 0.7978845608 * (
        1.0 + 0.134145 * pre * pre
    )
    return hidden, slope


def code(step):
    return (step[0] + 1) * 9 + (step[1] + 1) * 3 + step[2] + 1


def kernel(
    sizes,
    volume,
    w1,
    w2,
    w3,
    d1,
    d2,
    jv_out,
    gv1,
    gv2,
    *scratch,
):
    (rv, rp, rj, zv, zp, zj, ev, ep, ej, sv, sp, sj, slope_ref, back_ref,
     t1, t2, t3, shift, keep, acc, pack, land, part, full,
     hsend, hrecv, asend, arecv, bsend, brecv) = scratch
    depth, height, chan, width = volume.shape
    me = tuple(lax.axis_index(a) for a in AXES)
    total = sizes[0] * sizes[1] * sizes[2]
    line = (me[0] * sizes[1] + me[1]) * sizes[2] + me[2]

    def place(index):
        return (
            index // (sizes[1] * sizes[2]),
            index // sizes[2] % sizes[1],
            index % sizes[2],
        )

    barrier = pltpu.get_barrier_semaphore()

    @pl.loop(1, total)
    def _(i):
        pl.semaphore_signal(
            barrier, inc=1, device_id=place(lax.rem(line + i, total)), device_id_type=MESH
        )

    def there(step):
        ok = None
        for pos, size, delta in zip(me, sizes, step):
            if delta == -1:
                term = pos > 0
            elif delta == 1:
                term = pos < size - 1
            else:
                continue
            ok = term if ok is None else jnp.logical_and(ok, term)
        return ok

    def source(delta, extent):
        return {-1: pl.ds(1, 1), 1: pl.ds(extent, 1), 0: pl.ds(1, extent)}[delta]

    def target(delta, extent):
        return {-1: pl.ds(extent + 1, 1), 1: pl.ds(0, 1), 0: pl.ds(1, extent)}[delta]

    def landing(step, rows, zbuf):
        if step[2] == 0:
            return rows.at[target(step[0], depth), target(step[1], height)]
        return zbuf.at[0 if step[2] == 1 else 1, 1 - step[0], 1 - step[1]]

    def message(step, rows, zbuf, edge, slot):
        if step[2] == 0:
            src = rows.at[source(step[0], depth), source(step[1], height)]
        else:
            src = edge
        return pltpu.make_async_remote_copy(
            src_ref=src,
            dst_ref=landing(step, rows, zbuf),
            send_sem=hsend.at[slot, code(step)],
            recv_sem=hrecv.at[slot, code(step)],
            device_id=tuple(p + d for p, d in zip(me, step)),
            device_id_type=MESH,
        )

    def send(rows, zbuf, edge, slot, cross):
        for step in STEPS:
            if (step[2] != 0) == cross:

                @pl.when(there(step))
                def _():
                    message(step, rows, zbuf, edge, slot).start()

    def clear(rows, zbuf):
        for step in STEPS:
            back = tuple(-d for d in step)

            @pl.when(jnp.logical_not(there(back)))
            def _():
                ref = landing(step, rows, zbuf)
                ref[...] = jnp.zeros(ref.shape, ref.dtype)

    def receive(rows, zbuf, edge, slot, kind):
        for step in STEPS:
            if (step[0] != 0) != (kind == 1):
                continue
            back = tuple(-d for d in step)

            @pl.when(there(back))
            def _():
                message(step, rows, zbuf, edge, slot).wait_recv()

    def stage(rows, zbuf, edge, slot, out, table, group, finish):
        for kind in range(2):
            receive(rows, zbuf, edge, slot, kind)
            spread(rows, zbuf, out, (near, far)[kind])
            convolve(table, out, group, kind, finish)

    def sent(rows, zbuf, edge, slot):
        for step in STEPS:

            @pl.when(there(step))
            def _():
                message(step, rows, zbuf, edge, slot).wait_send()

    def edges(rows, edge):
        count = rows.shape[2]
        lane = lax.broadcasted_iota(jnp.int32, (count, width), 1)
        cells = depth * height
        built = jnp.zeros((count, width), jnp.float32)
        for x in range(depth):

            def step(y, built, x=x):
                row = rows[x + 1, y + 1].astype(jnp.float32)
                at = x * height + y
                built = jnp.where(lane == at, pltpu.roll(row, at, 1), built)
                return jnp.where(lane == cells + at, pltpu.roll(row, cells + at + 1, 1), built)

            built = lax.fori_loop(0, height, step, built, unroll=4)
        edge[...] = built.astype(edge.dtype)

    def shifter():
        src = lax.broadcasted_iota(jnp.int32, (2 * width, 2 * width), 0)
        dst = lax.broadcasted_iota(jnp.int32, (2 * width, 2 * width), 1)
        cells = depth * height
        low = jnp.logical_or(
            jnp.logical_and(src == dst - 1, src < width - 1),
            jnp.logical_and(
                dst == 0, jnp.logical_and(src >= width + cells, src < width + 2 * cells)
            ),
        )
        high = jnp.logical_or(
            jnp.logical_and(src == dst - width + 1, src < width),
            jnp.logical_and(
                dst == 2 * width - 1, jnp.logical_and(src >= width, src < width + cells)
            ),
        )
        pick = jnp.logical_or(
            jnp.logical_and(dst < width, low), jnp.logical_and(dst >= width, high)
        )
        shift[...] = jnp.where(pick, 1.0, 0.0).astype(shift.dtype)

    near = tuple(range(1, depth + 1))
    far = (0, depth + 1)

    def spread(rows, zbuf, out, planes):
        count = rows.shape[2]
        groups = count // chan
        lane = lax.broadcasted_iota(jnp.int32, (count, width), 1)
        cells = depth * height

        for xp in planes:
            dx = 0 if xp == 0 else (2 if xp == depth + 1 else 1)
            halo = []
            for yp in range(height + 2):
                dy = 0 if yp == 0 else (2 if yp == height + 1 else 1)
                left = zbuf[0, dx, dy].astype(jnp.float32)
                right = zbuf[1, dx, dy].astype(jnp.float32)
                at = (xp - 1) % depth * height + (yp - 1) % height
                both = jnp.where(lane == at, right, jnp.where(lane == cells + at, left, 0.0))
                halo.append(both.astype(rows.dtype))
            wide = rows[xp].reshape((height + 2) * count, width)
            lhs = jnp.concatenate([wide, jnp.concatenate(halo, axis=0)], axis=1)
            moved = jnp.dot(lhs, shift[...], preferred_element_type=jnp.float32)
            moved = moved.astype(rows.dtype).reshape(height + 2, count, 2 * width)
            kept = wide.reshape(height + 2, count, width)
            for g in range(groups):
                at = slice(g * chan, (g + 1) * chan)
                base = g * 3 * chan
                out[xp, :, base : base + chan] = moved[:, at, :width]
                out[xp, :, base + chan : base + 2 * chan] = kept[:, at]
                out[xp, :, base + 2 * chan : base + 3 * chan] = moved[:, at, width:]

    def band(weights, table, group):
        outs = weights.shape[0]
        third = weights.shape[1] // 3
        step = third // 3
        table[...] = jnp.zeros_like(table)
        for kx in range(3):
            piece = weights[:, kx * third : (kx + 1) * third]
            for ox in range(depth):
                xp = ox + kx
                kind, pos = (0, near.index(xp)) if xp in near else (1, far.index(xp))
                for oy in range(group):
                    row = (ox * group + oy) * outs
                    at = (pos * (group + 2) + oy) * step
                    table[kind, row : row + outs, at : at + third] = piece

    def convolve(table, ref, group, kind, finish):
        outs = table.shape[1] // (depth * group)
        planes = (near, far)[kind]

        @pl.loop(0, height // (2 * group))
        def _(j):
            halves = []
            for half in range(2):
                y = (2 * j + half) * group
                halves.append(
                    jnp.concatenate(
                        [
                            ref[xp, pl.ds(y, group + 2)].reshape(
                                (group + 2) * ref.shape[2], width
                            )
                            for xp in planes
                        ],
                        axis=0,
                    )
                )
            rhs = jnp.concatenate(halves, axis=1)
            out = jnp.dot(
                table[kind, :, : rhs.shape[0]], rhs, preferred_element_type=jnp.float32
            )
            if kind == 0:
                keep[j] = out
                return
            out = out + keep[j]
            for half in range(2):
                for ox in range(depth):
                    for oy in range(group):
                        row = (ox * group + oy) * outs
                        finish(
                            ox,
                            (2 * j + half) * group + oy,
                            out[row : row + outs, half * width : (half + 1) * width],
                        )

    def correlate(ref, rows, offset):
        acc[...] = jnp.zeros_like(acc)
        for x in range(depth):

            @pl.loop(0, height // 4)
            def _(j, x=x):
                y = 4 * j
                rhs = jnp.concatenate(
                    [rows[x + offset, y + i + offset] for i in range(4)], axis=1
                )
                for kx in range(3):
                    lhs = jnp.concatenate(
                        [
                            ref[x + kx, pl.ds(y + i, 3), : 3 * chan].reshape(9 * chan, width)
                            for i in range(4)
                        ],
                        axis=1,
                    )
                    acc[kx] += lax.dot_general(lhs, rhs, NT, preferred_element_type=jnp.float32)

    tiles = pack.shape[1]
    cells_all = float(depth * height * width * total)
    factor = math.sqrt(27.0 * chan)

    def owner(t):
        return t * total // tiles

    span = 8 * tiles
    lanes = width // chan

    def scatter(slot):
        for j in range(lanes):
            flat = acc[...].reshape(27 * chan, chan)
            pack[slot, :, :, j * chan : (j + 1) * chan] = flat[
                j * span : (j + 1) * span
            ].reshape(tiles, 8, chan)
        for t in range(tiles):
            at = owner(t)

            @pl.when(line != at)
            def _():
                pltpu.make_async_remote_copy(
                    src_ref=pack.at[slot, t],
                    dst_ref=land.at[slot, lax.rem(line - at + total, total) - 1],
                    send_sem=asend.at[slot],
                    recv_sem=arecv.at[slot],
                    device_id=place(at),
                    device_id_type=MESH,
                ).start()

    def gather(slot):
        for t in range(tiles):

            @pl.when(line == owner(t))
            def _():
                pltpu.make_async_copy(
                    land.at[slot], land.at[slot], arecv.at[slot]
                ).wait()
                summed = pack[slot, t] + jnp.sum(land[slot], axis=0)
                part[slot] = summed
                full[slot, t] = summed

                @pl.loop(1, total)
                def _(i):
                    pltpu.make_async_remote_copy(
                        src_ref=part.at[slot],
                        dst_ref=full.at[slot, t],
                        send_sem=bsend.at[slot],
                        recv_sem=brecv.at[slot],
                        device_id=place(lax.rem(line + i, total)),
                        device_id_type=MESH,
                    ).start()

    def owning():
        held = line == owner(0)
        for t in range(1, tiles):
            held = jnp.logical_or(held, line == owner(t))
        return held

    def drain(slot, out, direction):
        held = owning()
        for flag, count in ((held, tiles - 1), (jnp.logical_not(held), tiles)):

            @pl.when(flag)
            def _():
                some = full.at[slot, pl.ds(0, count)]
                pltpu.make_async_copy(some, some, brecv.at[slot]).wait()
                mine = pack.at[slot, pl.ds(0, count)]
                pltpu.make_async_copy(mine, mine, asend.at[slot]).wait()

        @pl.when(held)
        def _():
            pltpu.make_async_copy(land.at[slot], land.at[slot], bsend.at[slot]).wait()

        whole = full[slot].reshape(span, width)
        for j in range(lanes):
            at = slice(j * span, (j + 1) * span)
            damp = 0.1 * direction[at].astype(jnp.float32)
            out[at] = factor * (whole[:, j * chan : (j + 1) * chan] / cells_all + damp)

    inner = (slice(1, depth + 1), slice(1, height + 1))
    rv[inner] = volume[...]
    edges(rv, ev)
    for rows, zbuf in ((rv, zv), (rp, zp), (rj, zj)):
        clear(rows, zbuf)
    pl.semaphore_wait(barrier, total - 1)
    send(rv, zv, ev, 0, False)
    send(rv, zv, ev, 0, True)
    shifter()
    band(w1, t1, 2)
    band(w2, t2, 4)
    band(w3, t3, 4)

    def first(x, y, out):
        hidden, slope = gelu_pair(out[:chan])
        slope_ref[x, y] = slope
        rp[x + 1, y + 1, :chan] = hidden.astype(jnp.bfloat16)
        rp[x + 1, y + 1, chan:] = (slope * out[chan:]).astype(jnp.bfloat16)

    stage(rv, zv, ev, 0, sv, t1, 2, first)
    send(rp, zp, ep, 1, False)
    edges(rp, ep)
    send(rp, zp, ep, 1, True)

    def second(x, y, out):
        rj[x + 1, y + 1] = out.astype(jnp.bfloat16)

    stage(rp, zp, ep, 1, sp, t2, 4, second)
    send(rj, zj, ej, 2, False)
    edges(rj, ej)
    send(rj, zj, ej, 2, True)
    jv_out[...] = rj[inner]
    correlate(sp, rj, 1)
    scatter(0)

    def third(x, y, out):
        back_ref[x, y] = (slope_ref[x, y] * out).astype(jnp.bfloat16)

    stage(rj, zj, ej, 2, sj, t3, 4, third)
    gather(0)
    correlate(sv, back_ref, 0)
    scatter(1)
    gather(1)
    drain(0, gv2, d2)
    drain(1, gv1, d1)
    sent(rv, zv, ev, 0)
    sent(rp, zp, ep, 1)
    sent(rj, zj, ej, 2)


def body(volume, w_first, w_second, v_first, v_second):
    chan, depth, height, width = volume.shape
    sizes = tuple(lax.axis_size(a) for a in AXES)
    total = sizes[0] * sizes[1] * sizes[2]
    filt = 27 * chan
    tiles = filt * chan // (8 * width)
    w1 = jnp.concatenate([w_first, v_first], axis=-1).reshape(filt, 2 * chan).T
    w2 = jnp.stack([v_second, w_second], axis=2).reshape(2 * filt, chan).T
    w3 = jnp.transpose(jnp.flip(w_second, (0, 1, 2)), (3, 0, 1, 2, 4)).reshape(chan, filt)
    cells = jnp.transpose(volume, (1, 2, 0, 3))
    bf, f32 = jnp.bfloat16, jnp.float32
    pads = (depth + 2, height + 2)
    vmem = pl.BlockSpec(memory_space=pltpu.VMEM)
    jv, corr1, corr2 = pl.pallas_call(
        functools.partial(kernel, sizes),
        out_shape=(
            jax.ShapeDtypeStruct((depth, height, chan, width), bf),
            jax.ShapeDtypeStruct((filt, chan), f32),
            jax.ShapeDtypeStruct((filt, chan), f32),
        ),
        in_specs=[vmem] * 6,
        out_specs=(vmem,) * 3,
        scratch_shapes=[
            pltpu.VMEM(pads + (chan, width), bf),
            pltpu.VMEM(pads + (2 * chan, width), bf),
            pltpu.VMEM(pads + (chan, width), bf),
            pltpu.VMEM((2, 3, 3, chan, width), bf),
            pltpu.VMEM((2, 3, 3, 2 * chan, width), bf),
            pltpu.VMEM((2, 3, 3, chan, width), bf),
            pltpu.VMEM((chan, width), bf),
            pltpu.VMEM((2 * chan, width), bf),
            pltpu.VMEM((chan, width), bf),
            pltpu.VMEM(pads + (3 * chan, width), bf),
            pltpu.VMEM(pads + (6 * chan, width), bf),
            pltpu.VMEM(pads + (3 * chan, width), bf),
            pltpu.VMEM((depth, height, chan, width), f32),
            pltpu.VMEM((depth, height, chan, width), bf),
            pltpu.VMEM((2, depth * 2 * 2 * chan, depth * 4 * 3 * chan), bf),
            pltpu.VMEM((2, depth * 4 * chan, depth * 6 * 6 * chan), bf),
            pltpu.VMEM((2, depth * 4 * chan, depth * 6 * 3 * chan), bf),
            pltpu.VMEM((2 * width, 2 * width), bf),
            pltpu.VMEM((height // 4, depth * 4 * chan, 2 * width), f32),
            pltpu.VMEM((3, 9 * chan, chan), f32),
            pltpu.VMEM((2, tiles, 8, width), f32),
            pltpu.VMEM((2, total - 1, 8, width), f32),
            pltpu.VMEM((2, 8, width), f32),
            pltpu.VMEM((2, tiles, 8, width), f32),
            pltpu.SemaphoreType.DMA((3, 27)),
            pltpu.SemaphoreType.DMA((3, 27)),
            pltpu.SemaphoreType.DMA((2,)),
            pltpu.SemaphoreType.DMA((2,)),
            pltpu.SemaphoreType.DMA((2,)),
            pltpu.SemaphoreType.DMA((2,)),
        ],
        compiler_params=pltpu.CompilerParams(
            collective_id=0, has_side_effects=True, vmem_limit_bytes=48 * 1024 * 1024
        ),
    )(cells, w1, w2, w3, v_first.reshape(filt, chan), v_second.reshape(filt, chan))
    return (
        jnp.transpose(jv, (2, 0, 1, 3)),
        corr1.reshape(v_first.shape),
        corr2.reshape(v_second.shape),
    )


def solution(mesh):
    in_specs = (P(None, "gx", "gy", "gz"), P(), P(), P(), P())
    out_specs = (P(None, "gx", "gy", "gz"), P(), P())
    return jax.shard_map(body, mesh=mesh, in_specs=in_specs, out_specs=out_specs, check_vma=False)
```
